32 devices in a mesh: slab: 4 (over y, x), space: 8 (over z, core).
Axes of the slice: x: 2, y: 2, z: 4, core: 2. Of those that a mesh axis runs over, the one named last changes fastest.
Arguments:
- dipoles: float32 [3, 16384], P(None, ('slab', 'space')), may hold values from -3 to 3
- residual: float32 [3, 16384], P(None, ('slab', 'space')), may hold values from -12 to 12, as said below
- cells: int32 [3, 16384], P(None, ('slab', 'space')), may hold values from 0 to 255, as said below
- fraction: float32 [3, 16384], P(None, ('slab', 'space')), may hold values from 0.25 to 0.75
- polarizability: float32 [16384], P(('slab', 'space')), may hold values from 0.3 to 2.5
- tile_order: int32 [32, 512], P(('slab', 'space')), may hold values from 0 to 511, as said below
- send_tiles: int32 [32, 2], P(('slab', 'space')), may hold values from 0 to 3, as said below
- tile_lists: int32 [32, 4, 8], P(('slab', 'space')), may hold values from 0 to 19, as said below
- tile_counts: int32 [32, 4], P(('slab', 'space')), may hold values from 1 to 8, as said below
Outputs:
- dipoles_next: float32 [3, 16384], P(None, ('slab', 'space'))
- residual_next: float32 [3, 16384], P(None, ('slab', 'space'))
- direction: float32 [3, 16384], P(None, ('slab', 'space'))
The draws below stay inside these ranges and needn't reach their ends.
Inputs may be any that keep to these rules, and one draw needn't show every extreme that they name: The residual's entries stay within the stated range. `cells`: the first component is below 64 and the second below 32; no two atoms of one device share a cell. `tile_order`: each device's row holds every number of 0 to 511 once. `send_tiles`: the 2 tile numbers of each device are distinct. `tile_lists`: entry 0 of the list of tile t is t itself; the 8 entries of one list are distinct. `tile_counts`: on some devices every tile has 8 live entries.
All inputs are finite; a program needn't handle non-finite values.
Results may differ from the reference program's by a relative error of at most 0.0003.
Values sent between devices are 32-bit elements; how exact they have to be, the bound alone decides.
A program may use at most 128 MiB of HBM per device.

```python
import math
import jax
import jax.numpy as jnp
from jax import lax

G = 256
TILE = 128
TILES_DEV = 4
MAXN = 8
XL = 64
YL = 32
SEND = 2
POOL = 20
ATOM_DEV = 512
ATOMS = 16384
N_SLAB = 4
N_SPACE = 8
DEVICES = 32


def tile_layout():
    aspect_ratio = max(G // XL, 1)
    tiles_across = 1
    for doubling in range(6):
        candidate = tiles_across * 2
        if TILES_DEV % candidate == 0 and candidate * candidate * aspect_ratio <= TILES_DEV:
            tiles_across = candidate
    tiles_depth = TILES_DEV // tiles_across
    return (tiles_depth, XL // tiles_across, G // tiles_depth)


def atom_layout(key):
    tiles_depth, box_width, box_depth = tile_layout()
    box_cells = box_width * YL * box_depth
    device_keys = jax.random.split(jax.random.fold_in(key, 101), DEVICES)
    tile_ids = jnp.arange(TILES_DEV, dtype=jnp.int32)
    anchor_x = tile_ids // tiles_depth * box_width
    anchor_z = tile_ids % tiles_depth * box_depth

    def one_tile(tile_key):
        return jax.random.permutation(tile_key, box_cells)[:TILE]

    def one_device(device_key):
        order_key, place_key = jax.random.split(device_key)
        ordering = jax.random.permutation(order_key, ATOM_DEV).astype(jnp.int32)
        picked = jax.vmap(one_tile)(jax.random.split(place_key, TILES_DEV)).astype(jnp.int32)
        cell_x = anchor_x[:, None] + picked // (YL * box_depth)
        cell_y = picked // box_depth % YL
        cell_z = anchor_z[:, None] + picked % box_depth
        ordered = jnp.stack([cell_x, cell_y, cell_z]).reshape(3, ATOM_DEV)
        placed = jnp.zeros((3, ATOM_DEV), jnp.int32).at[:, ordering].set(ordered)
        return (ordering, placed)
    orderings, placed = jax.vmap(one_device)(device_keys)
    return (orderings.astype(jnp.int32), jnp.transpose(placed, (1, 0, 2)).reshape(3, ATOMS).astype(jnp.int32))


def shared_tiles(key):
    device_keys = jax.random.split(jax.random.fold_in(key, 202), DEVICES)

    def one_device(device_key):
        return jax.random.permutation(device_key, TILES_DEV)[:SEND]
    return jax.vmap(one_device)(device_keys).astype(jnp.int32)


def draw_residual(key, part):
    device_rank = (jnp.arange(ATOMS) // ATOM_DEV).astype(jnp.float32) / max(DEVICES - 1, 1)
    rising = 1.0 + 2.0 * device_rank
    samples = jnp.clip(jax.random.normal(key, (3, ATOMS), jnp.float32), -4.0, 4.0)
    return samples * rising[None]


def draw_cells(key, part):
    return atom_layout(key)[1]


def draw_tile_order(key, part):
    return atom_layout(key)[0]


def draw_send_tiles(key, part):
    return shared_tiles(key)


def draw_tile_lists(key, part):
    tiles_depth, box_width, box_depth = tile_layout()
    sending = shared_tiles(key)
    count_slab = G // XL
    count_space = G // YL
    device_ids = jnp.arange(DEVICES, dtype=jnp.int32)
    slab_ids = device_ids // count_space
    space_ids = device_ids % count_space
    offset_a = jnp.array([0, 0, 0, 1, 1, 2, 2, 2], jnp.int32)
    offset_b = jnp.array([0, 1, 2, 0, 2, 0, 1, 2], jnp.int32)
    beside_all = (slab_ids[:, None] + offset_a[None] - 1 + count_slab) % count_slab * count_space + (space_ids[:, None] + offset_b[None] - 1 + count_space) % count_space
    remote = sending[beside_all].reshape(DEVICES, 8 * SEND)
    own_tiles = jnp.broadcast_to(jnp.arange(TILES_DEV, dtype=jnp.int32)[None], (DEVICES, TILES_DEV))
    pool_tiles = jnp.concatenate([own_tiles, remote], 1)
    shift_x = jnp.concatenate([jnp.zeros((TILES_DEV,), jnp.int32), jnp.repeat(offset_a - 1, SEND)]) * XL
    low_x = pool_tiles // tiles_depth * box_width + shift_x[None]
    low_z = pool_tiles % tiles_depth * box_depth
    apart_x = jnp.abs(low_x[:, None, :] - low_x[:, :TILES_DEV, None])
    gap_x = jnp.maximum(apart_x - box_width, 0)
    apart_z = (low_z[:, None, :] - low_z[:, :TILES_DEV, None]) % G
    apart_z = jnp.minimum(apart_z, G - apart_z)
    gap_z = jnp.maximum(apart_z - box_depth, 0)
    rank_keys = jax.random.split(jax.random.fold_in(key, 303), DEVICES * TILES_DEV)

    def one_rank(rank_key):
        return jax.random.permutation(rank_key, POOL)
    ranks = jax.vmap(one_rank)(rank_keys).reshape(DEVICES, TILES_DEV, POOL).astype(jnp.int32)
    scores = (gap_x * gap_x + gap_z * gap_z) * POOL + ranks
    itself = jnp.arange(POOL, dtype=jnp.int32)[None, None, :] == jnp.arange(TILES_DEV, dtype=jnp.int32)[None, :, None]
    scores = jnp.where(itself, -1, scores)
    ordering = jnp.argsort(scores, axis=2, stable=True)
    return ordering[:, :, :MAXN].astype(jnp.int32)


def draw_tile_counts(key, part):
    first_key, second_key = jax.random.split(jax.random.fold_in(key, 5))
    heavy = jax.random.randint(first_key, (DEVICES, 1), 0, 8) == 0
    heavy = heavy.at[0].set(True)
    light = jax.random.randint(second_key, (DEVICES, TILES_DEV), 1, MAXN // 2 + 1)
    return jnp.where(heavy, MAXN, light).astype(jnp.int32)


def shard_levels(rng, dims, shards, smallest, largest):
    gain = 1.0
    for position, blocks in shards:
        heights = jax.random.uniform(jax.random.fold_in(jax.random.fold_in(rng, 6), position), (blocks,), jnp.float32, smallest / len(shards), largest / len(shards))
        gain = gain * jnp.repeat(jnp.exp(heights), dims[position] // blocks).reshape((-1,) + (1,) * (len(dims) - 1 - position))
    return gain


def centred(rng, extent, deviation, most, pieces=(), held_as=jnp.bfloat16):
    drawn = jax.random.normal(rng, extent, jnp.float32) * deviation
    if len(pieces) > 0:
        drawn = shard_levels(rng, extent, pieces, -0.22, 0.18) * drawn
    return jnp.clip(drawn, min=-most, max=most).astype(held_as)


def setup_inputs(seed: int = 0) -> dict:
    streams_of = jax.random.split(jax.random.key(seed), 10)
    return {
        "dipoles": centred(streams_of[0], (3, ATOMS), 0.5, 3.0, ((1, 32),), jnp.float32),
        "residual": draw_residual(jax.random.fold_in(streams_of[9], 71), 0),
        "cells": draw_cells(jax.random.fold_in(streams_of[9], 71), 0),
        "fraction": jnp.clip(0.25 + 0.5 * jax.random.uniform(streams_of[3], (3, ATOMS), jnp.float32) ** shard_levels(streams_of[3], (3, ATOMS), ((1, 32),), -0.2, 0.2), 0.25, 0.75),
        "polarizability": jnp.clip(jnp.exp(math.log(2.5) - 2.1202635 * jax.random.uniform(streams_of[4], (ATOMS,), jnp.float32) ** shard_levels(streams_of[4], (ATOMS,), ((0, 32),), -0.2, 0.2)), 0.3, 2.5),
        "tile_order": draw_tile_order(jax.random.fold_in(streams_of[9], 71), 0),
        "send_tiles": draw_send_tiles(jax.random.fold_in(streams_of[9], 71), 0),
        "tile_lists": draw_tile_lists(jax.random.fold_in(streams_of[9], 71), 0),
        "tile_counts": draw_tile_counts(jax.random.fold_in(streams_of[9], 71), 0),
    }


EWALD_BETA = 0.4
THOLE_SCALE = 0.39
SELF_FIELD = 4.0 * EWALD_BETA ** 3 / (3.0 * math.sqrt(math.pi))

def spline(fraction):
    centre_arg = fraction - 0.5
    lower_one = fraction + 0.5
    upper_one = 1.5 - fraction
    lower_two = fraction + 1.5
    upper_two = 2.5 - fraction

    def middle(amount):
        return (55.0 + 20.0 * amount - 120.0 * amount ** 2 + 80.0 * amount ** 3 - 16.0 * amount ** 4) / 96.0

    def middle_slope(amount):
        return (20.0 - 240.0 * amount + 240.0 * amount ** 2 - 64.0 * amount ** 3) / 96.0

    def outer_piece(amount):
        return (5.0 - 2.0 * amount) ** 4 / 384.0

    def outer_slope(amount):
        return -(5.0 - 2.0 * amount) ** 3 / 48.0
    centre = 115.0 / 192.0 - 0.625 * centre_arg ** 2 + 0.25 * centre_arg ** 4
    centre_slope = -1.25 * centre_arg + centre_arg ** 3
    weights = jnp.stack([outer_piece(lower_two), middle(lower_one), centre, middle(upper_one), outer_piece(upper_two)])
    slopes = jnp.stack([outer_slope(lower_two), middle_slope(lower_one), centre_slope, -middle_slope(upper_one), -outer_slope(upper_two)])
    return (weights, slopes)

def wave_factors(freq_ids):
    wrapped = jnp.where(freq_ids > G // 2, freq_ids - G, freq_ids).astype(jnp.float32) / G
    angles = 2.0 * math.pi / G * freq_ids.astype(jnp.float32)
    modulus = 115.0 / 192.0 + 19.0 / 48.0 * jnp.cos(angles) + 1.0 / 192.0 * jnp.cos(2.0 * angles)
    return (wrapped * wrapped, jnp.exp(-(math.pi / EWALD_BETA) ** 2 * wrapped * wrapped) / (modulus * modulus))

def multiplier(freq_x, freq_y, freq_z):
    square_x, factor_x = wave_factors(freq_x)
    square_y, factor_y = wave_factors(freq_y)
    square_z, factor_z = wave_factors(freq_z)
    square_sum = square_x + square_y + square_z
    anchor = ((freq_x == 0) & (freq_y == 0) & (freq_z == 0)).astype(jnp.float32)
    return (1.0 - anchor) * factor_x * factor_y * factor_z / (math.pi * float(G) ** 3 * (square_sum + anchor))

def short_field(own_geometry, pool_geometry, pool_dipoles, neighbour_ids, neighbour_counts):
    count_tiles = own_geometry.shape[0]
    tile_width = own_geometry.shape[2]
    slots = neighbour_ids.shape[1]
    tile_ids = jnp.arange(count_tiles, dtype=jnp.int32)
    diagonal = (jnp.arange(tile_width)[:, None] == jnp.arange(tile_width)[None, :]).astype(jnp.float32)
    slot_ids = jnp.arange(slots, dtype=jnp.int32)

    def per_tile(inputs):
        tile_id, own_tile, picked, live_count = inputs
        geometry = pool_geometry[picked]
        dipole = pool_dipoles[picked]
        displacement = geometry[:, :3, None, :] - own_tile[None, :3, :, None]
        half_box = 0.5 * G
        depth_z = displacement[:, 2]
        depth_z = jnp.where(depth_z > half_box, depth_z - G, jnp.where(depth_z < -half_box, depth_z + G, depth_z))
        displacement = jnp.stack([displacement[:, 0], displacement[:, 1], depth_z], 1)
        itself = (picked == tile_id).astype(jnp.float32)[:, None, None] * diagonal[None]
        square = lax.optimization_barrier(jnp.sum(displacement * displacement, 1)) + itself
        distance = jnp.sqrt(square)
        inverse = 1.0 / distance
        inverse_sq = inverse * inverse
        gauss = jnp.exp(-EWALD_BETA ** 2 * square)
        bare_zero = lax.erfc(EWALD_BETA * distance) * inverse
        bare_one = (bare_zero + 2.0 * EWALD_BETA / math.sqrt(math.pi) * gauss) * inverse_sq
        bare_two = (3.0 * bare_one + 4.0 * EWALD_BETA ** 3 / math.sqrt(math.pi) * gauss) * inverse_sq
        damping = THOLE_SCALE * square * distance * lax.rsqrt(own_tile[3][None, :, None] * geometry[:, 3][:, None, :])
        decay = jnp.exp(-damping)
        rank_three = bare_one - decay * inverse * inverse_sq
        rank_five = bare_two - 3.0 * (1.0 + damping) * decay * inverse * inverse_sq * inverse_sq
        weight_pair = (slot_ids < live_count).astype(jnp.float32)[:, None, None] * (1.0 - itself)
        projection = lax.optimization_barrier(jnp.sum(displacement * dipole[:, :, None, :], 1))
        terms = rank_five[:, None] * displacement * projection[:, None] - rank_three[:, None] * dipole[:, :, None, :]
        return lax.optimization_barrier(jnp.sum(weight_pair[:, None] * terms, (0, 3)))
    return lax.map(per_tile, (tile_ids, own_geometry, neighbour_ids, neighbour_counts))

def tiled(values, tile_order):
    channels = values.shape[0]
    blocks = values.reshape(channels, DEVICES, ATOM_DEV).transpose(1, 0, 2)
    ordered = jnp.take_along_axis(blocks, tile_order[:, None, :], axis=2)
    return ordered.reshape(DEVICES, channels, TILES_DEV, TILE).transpose(0, 2, 1, 3)

def untiled(tile_values, tile_order):
    channels = tile_values.shape[2]
    ordered = tile_values.transpose(0, 2, 1, 3).reshape(DEVICES, channels, ATOM_DEV)

    def restore(row_values, row_order):
        return jnp.zeros_like(row_values).at[:, row_order].set(row_values)
    blocks = jax.vmap(restore)(ordered, tile_order)
    return blocks.transpose(1, 0, 2).reshape(channels, ATOMS)

def recip_field(direction, cells, fraction):
    device_ids = jnp.arange(ATOMS, dtype=jnp.int32) // ATOM_DEV
    base_x = cells[0] + device_ids // N_SPACE * XL
    base_y = cells[1] + device_ids % N_SPACE * YL
    base_z = cells[2]
    weight_x, slope_x = spline(fraction[0])
    weight_y, slope_y = spline(fraction[1])
    weight_z, slope_z = spline(fraction[2])
    points_z = (base_z[None] + jnp.arange(5, dtype=jnp.int32)[:, None] - 2 + G) % G
    density = jnp.zeros((G, G, G), jnp.float32)
    for step_x in range(5):
        for step_y in range(5):
            points_x = (base_x + step_x - 2 + G) % G
            points_y = (base_y + step_y - 2 + G) % G
            values = (direction[0] * slope_x[step_x] * weight_y[step_y])[None] * weight_z
            values = values + (direction[1] * weight_x[step_x] * slope_y[step_y])[None] * weight_z
            values = values + (direction[2] * weight_x[step_x] * weight_y[step_y])[None] * slope_z
            density = density.at[points_x[None], points_y[None], points_z].add(values)
    freq_ids = jnp.arange(G, dtype=jnp.int32)
    factor = multiplier(freq_ids[:, None, None], freq_ids[None, :, None], freq_ids[None, None, :])
    potential = jnp.real(jnp.fft.ifftn(factor * jnp.fft.fftn(density))) * float(G) ** 3
    field_x = jnp.zeros((ATOMS,), potential.dtype)
    field_y = jnp.zeros((ATOMS,), potential.dtype)
    field_z = jnp.zeros((ATOMS,), potential.dtype)
    for step_x in range(5):
        for step_y in range(5):
            points_x = (base_x + step_x - 2 + G) % G
            points_y = (base_y + step_y - 2 + G) % G
            values = potential[points_x[None], points_y[None], points_z]
            field_x = field_x - lax.optimization_barrier(jnp.sum((slope_x[step_x] * weight_y[step_y])[None] * weight_z * values, 0))
            field_y = field_y - lax.optimization_barrier(jnp.sum((weight_x[step_x] * slope_y[step_y])[None] * weight_z * values, 0))
            field_z = field_z - lax.optimization_barrier(jnp.sum((weight_x[step_x] * weight_y[step_y])[None] * slope_z * values, 0))
    return jnp.stack([field_x, field_y, field_z])

def reference(dipoles, residual, cells, fraction, polarizability, tile_order, send_tiles, tile_lists, tile_counts):
    positions = cells.astype(jnp.float32) + fraction
    geometry_tiles = tiled(jnp.concatenate([positions, polarizability[None]], 0), tile_order)
    device_ids = jnp.arange(DEVICES, dtype=jnp.int32)
    slab_ids = device_ids // N_SPACE
    space_ids = device_ids % N_SPACE
    beside_all = [(step_a, step_b) for step_a in range(3) for step_b in range(3) if (step_a, step_b) != (1, 1)]
    neighbours = jnp.stack([(slab_ids + step_a - 1 + N_SLAB) % N_SLAB * N_SPACE + (space_ids + step_b - 1 + N_SPACE) % N_SPACE for step_a, step_b in beside_all], 1)
    shifts = jnp.array([[float((step_a - 1) * XL), float((step_b - 1) * YL), 0.0, 0.0] for step_a, step_b in beside_all], jnp.float32)
    sent_geometry = jnp.take_along_axis(geometry_tiles, send_tiles[:, :, None, None], axis=1)

    def short(values):
        dipole_tiles = tiled(values, tile_order)
        sent_dipoles = jnp.take_along_axis(dipole_tiles, send_tiles[:, :, None, None], axis=1)

        def per_device(device):
            near = neighbours[device]
            pool_geometry = jnp.concatenate([geometry_tiles[device], (sent_geometry[near] + shifts[:, None, :, None]).reshape(8 * SEND, 4, TILE)], 0)
            pool_dipoles = jnp.concatenate([dipole_tiles[device], sent_dipoles[near].reshape(8 * SEND, 3, TILE)], 0)
            return short_field(geometry_tiles[device], pool_geometry, pool_dipoles, tile_lists[device], tile_counts[device])
        return untiled(lax.map(per_device, device_ids), tile_order)
    alphas = polarizability[None]
    search = alphas * residual
    for sweep_id in range(3):
        search = alphas * (residual + short(search))
    direction = search
    search_dot = jnp.sum(residual * direction)
    applied = direction / alphas - short(direction) - SELF_FIELD * direction - recip_field(direction, cells, fraction)
    curve_total = jnp.sum(direction * applied)
    step_size = search_dot / curve_total
    return (dipoles + step_size * direction, residual - step_size * applied, direction)
```

```python
import functools
import math

import jax
import jax.numpy as jnp
from jax import lax
from jax.experimental import pallas as pl
from jax.experimental.pallas import tpu as pltpu
from jax.sharding import PartitionSpec as P

G = 256


EWALD_BETA = 0.4
THOLE_SCALE = 0.39
SELF_FIELD = 4.0 * EWALD_BETA**3 / (3.0 * math.sqrt(math.pi))
HIGHEST = lax.Precision.HIGHEST


def with_halo(array, sides, width):
    for axis, dim in sides:
        devices, length = (lax.axis_size(axis), array.shape[dim])
        up = [(i, (i + 1) % devices) for i in range(devices)]
        down = [(j, i) for i, j in up]
        last = lax.slice_in_dim(array, length - width, length, axis=dim)
        initial = lax.slice_in_dim(array, 0, width, axis=dim)
        before = lax.ppermute(last, axis, up)
        after = lax.ppermute(initial, axis, down)
        array = jnp.concatenate([before, array, after], axis=dim)
    return array


def spline(fraction):
    centre_arg = fraction - 0.5
    lower_one = fraction + 0.5
    upper_one = 1.5 - fraction
    lower_two = fraction + 1.5
    upper_two = 2.5 - fraction

    def middle(amount):
        return (
            55.0 + 20.0 * amount - 120.0 * amount**2 + 80.0 * amount**3 - 16.0 * amount**4
        ) / 96.0

    def middle_slope(amount):
        return (20.0 - 240.0 * amount + 240.0 * amount**2 - 64.0 * amount**3) / 96.0

    def outer_piece(amount):
        return (5.0 - 2.0 * amount) ** 4 / 384.0

    def outer_slope(amount):
        return -((5.0 - 2.0 * amount) ** 3) / 48.0

    centre = 115.0 / 192.0 - 0.625 * centre_arg**2 + 0.25 * centre_arg**4
    centre_slope = -1.25 * centre_arg + centre_arg**3
    weights = jnp.stack(
        [
            outer_piece(lower_two),
            middle(lower_one),
            centre,
            middle(upper_one),
            outer_piece(upper_two),
        ]
    )
    slopes = jnp.stack(
        [
            outer_slope(lower_two),
            middle_slope(lower_one),
            centre_slope,
            -middle_slope(upper_one),
            -outer_slope(upper_two),
        ]
    )
    return (weights, slopes)


def wave_factors(freq_ids):
    wrapped = jnp.where(freq_ids > G // 2, freq_ids - G, freq_ids).astype(jnp.float32) / G
    angles = 2.0 * math.pi / G * freq_ids.astype(jnp.float32)
    modulus = 115.0 / 192.0 + 19.0 / 48.0 * jnp.cos(angles) + 1.0 / 192.0 * jnp.cos(2.0 * angles)
    return (
        wrapped * wrapped,
        jnp.exp(-((math.pi / EWALD_BETA) ** 2) * wrapped * wrapped) / (modulus * modulus),
    )


def multiplier(freq_x, freq_y, freq_z):
    square_x, factor_x = wave_factors(freq_x)
    square_y, factor_y = wave_factors(freq_y)
    square_z, factor_z = wave_factors(freq_z)
    square_sum = square_x + square_y + square_z
    anchor = ((freq_x == 0) & (freq_y == 0) & (freq_z == 0)).astype(jnp.float32)
    return (
        (1.0 - anchor)
        * factor_x
        * factor_y
        * factor_z
        / (math.pi * float(G) ** 3 * (square_sum + anchor))
    )


def separation(own_tile, geometry):
    displacement = geometry[:, :3, None, :] - own_tile[None, :3, :, None]
    half_box = 0.5 * G
    depth_z = displacement[:, 2]
    depth_z = jnp.where(
        depth_z > half_box, depth_z - G, jnp.where(depth_z < -half_box, depth_z + G, depth_z)
    )
    return jnp.stack([displacement[:, 0], displacement[:, 1], depth_z], 1)


def grouped(values, group_count):
    return values.reshape((group_count, -1) + values.shape[1:])


def pair_coefficients(own_geometry, pool_geometry, neighbour_ids, neighbour_counts):
    count_tiles = own_geometry.shape[0]
    tile_width = own_geometry.shape[2]
    slots = neighbour_ids.shape[1]
    group_count = count_tiles // math.gcd(count_tiles, 4)
    tile_ids = jnp.arange(count_tiles, dtype=jnp.int32)
    diagonal = (jnp.arange(tile_width)[:, None] == jnp.arange(tile_width)[None, :]).astype(
        jnp.float32
    )
    slot_ids = jnp.arange(slots, dtype=jnp.int32)

    def pair_per_tile(tile_id, own_tile, picked, live_count):
        geometry = pool_geometry[picked]
        displacement = separation(own_tile, geometry)
        itself = (picked == tile_id).astype(jnp.float32)[:, None, None] * diagonal[None]
        square = jnp.sum(displacement * displacement, 1) + itself
        distance = jnp.sqrt(square)
        inverse = 1.0 / distance
        inverse_sq = inverse * inverse
        gauss = jnp.exp(-(EWALD_BETA**2) * square)
        bare_zero = lax.erfc(EWALD_BETA * distance) * inverse
        bare_one = (bare_zero + 2.0 * EWALD_BETA / math.sqrt(math.pi) * gauss) * inverse_sq
        bare_two = (3.0 * bare_one + 4.0 * EWALD_BETA**3 / math.sqrt(math.pi) * gauss) * inverse_sq
        damping = (
            THOLE_SCALE
            * square
            * distance
            * lax.rsqrt(own_tile[3][None, :, None] * geometry[:, 3][:, None, :])
        )
        decay = jnp.exp(-damping)
        rank_three = bare_one - decay * inverse * inverse_sq
        rank_five = bare_two - 3.0 * (1.0 + damping) * decay * inverse * inverse_sq * inverse_sq
        weight_pair = (slot_ids < live_count).astype(jnp.float32)[:, None, None] * (1.0 - itself)
        return (weight_pair * rank_five, weight_pair * rank_three)

    def pair_per_group(inputs):
        return jax.vmap(pair_per_tile)(*inputs)

    fives, threes = lax.map(
        pair_per_group,
        (
            grouped(tile_ids, group_count),
            grouped(own_geometry, group_count),
            grouped(neighbour_ids, group_count),
            grouped(neighbour_counts, group_count),
        ),
    )
    return (
        fives.reshape((count_tiles,) + fives.shape[2:]),
        threes.reshape((count_tiles,) + threes.shape[2:]),
    )


def short_field(own_geometry, pool_geometry, pool_dipoles, neighbour_ids, coefficients):
    count_tiles = own_geometry.shape[0]
    group_count = count_tiles // math.gcd(count_tiles, 4)
    fives, threes = coefficients

    def short_per_tile(own_tile, picked, rank_five, rank_three):
        geometry = pool_geometry[picked]
        dipole = pool_dipoles[picked]
        displacement = separation(own_tile, geometry)
        projection = jnp.sum(displacement * dipole[:, :, None, :], 1)
        terms = (
            rank_five[:, None] * displacement * projection[:, None]
            - rank_three[:, None] * dipole[:, :, None, :]
        )
        return jnp.sum(terms, (0, 3))

    def short_per_group(inputs):
        return jax.vmap(short_per_tile)(*inputs)

    fields = lax.map(
        short_per_group,
        (
            grouped(own_geometry, group_count),
            grouped(neighbour_ids, group_count),
            grouped(fives, group_count),
            grouped(threes, group_count),
        ),
    )
    return fields.reshape((count_tiles,) + fields.shape[2:])


def to_tiles(values, count_tiles):
    return values.reshape(values.shape[0], count_tiles, -1).transpose(1, 0, 2)


def from_tiles(tile_values):
    return tile_values.transpose(1, 0, 2).reshape(tile_values.shape[1], -1)


def tile_rims(payload):
    return with_halo(payload, (("slab", 0), ("space", 1)), 1)


def pool_from(received):
    flattened = received.reshape((9,) + received.shape[2:])
    picked = flattened[jnp.array([0, 1, 2, 3, 5, 6, 7, 8], dtype=jnp.int32)]
    return picked.reshape((-1,) + received.shape[3:])


NT = (((1,), (1,)), ((), ()))
NN = (((1,), (0,)), ((), ()))


def dot3(left, right, dims):
    def halves(value):
        high = value.astype(jnp.bfloat16)
        return high, (value - high.astype(jnp.float32)).astype(jnp.bfloat16)

    left_high, left_low = halves(left)
    right_high, right_low = halves(right)
    dot = functools.partial(
        lax.dot_general, dimension_numbers=dims, preferred_element_type=jnp.float32
    )
    return dot(left_high, right_high) + (dot(left_high, right_low) + dot(left_low, right_high))


def window_tables(cell_row, frac_row, length):
    weights, slopes = spline(frac_row)
    offsets = lax.broadcasted_iota(jnp.int32, (length, cell_row.shape[1]), 0) - cell_row
    weight_table = jnp.zeros(offsets.shape, jnp.float32)
    slope_table = jnp.zeros(offsets.shape, jnp.float32)
    for step in range(5):
        matched = offsets == step
        weight_table = jnp.where(matched, weights[step], weight_table)
        slope_table = jnp.where(matched, slopes[step], slope_table)
    return weight_table, slope_table


def spread_kernel(cell_ref, frac_ref, search_ref, wave_ref, slope_wave_ref, cas_ref, out_ref):
    width_u, width_v = out_ref.shape[2], cas_ref.shape[1]
    freqs = wave_ref.shape[1]
    weight_x, slope_x = window_tables(cell_ref[0, 0:1], frac_ref[0, 0:1], width_u)
    weight_y, slope_y = window_tables(cell_ref[0, 1:2], frac_ref[0, 1:2], width_v)
    along_x = jnp.concatenate([slope_x, weight_x], 1)
    moved_x = search_ref[0, 0:1]
    moved_y = search_ref[0, 1:2]
    moved_z = search_ref[0, 2:3]
    rows = []
    for k in range(freqs):
        wave = wave_ref[0, k : k + 1]
        slope_wave = slope_wave_ref[0, k : k + 1]
        rows.append(
            jnp.concatenate(
                [
                    weight_y * (moved_x * wave),
                    slope_y * (moved_y * wave) + weight_y * (moved_z * slope_wave),
                ],
                1,
            )
        )
    spread = dot3(jnp.concatenate(rows, 0), along_x, NT)
    turned = jnp.concatenate(
        [spread[k * width_v : (k + 1) * width_v].T for k in range(freqs)], 0
    )
    along_y = dot3(turned, cas_ref[0], NN).reshape(freqs, width_u, -1)

    @pl.when(pl.program_id(1) == 0)
    def _():
        out_ref[:, 0] = along_y

    @pl.when(pl.program_id(1) > 0)
    def _():
        out_ref[:, 0] += along_y


def scale_kernel(planes_ref, cas_ref, turned_ref, factor_ref, out_ref, energy_ref):
    spectrum = dot3(turned_ref[...], planes_ref[0], NN)
    scaled = spectrum * factor_ref[0]
    energy = jnp.sum(scaled * spectrum, 0, keepdims=True)
    energy_ref[0] = jnp.broadcast_to(energy, energy_ref.shape[1:])
    out_ref[0] = dot3(cas_ref[...], scaled, NN)


def probe_kernel(cell_ref, frac_ref, planes_ref, wave_ref, slope_wave_ref, cas_ref, out_ref):
    width_u, width_v = planes_ref.shape[2], cas_ref.shape[1]
    freqs = wave_ref.shape[1]
    atoms = cell_ref.shape[2]
    weight_x, slope_x = window_tables(cell_ref[0, 0:1], frac_ref[0, 0:1], width_u)
    weight_y, slope_y = window_tables(cell_ref[0, 1:2], frac_ref[0, 1:2], width_v)
    along_x = jnp.concatenate([slope_x, weight_x], 1)
    planes = jnp.concatenate([dot3(cas_ref[0], planes_ref[k, 0], NT) for k in range(freqs)], 0)
    probed = dot3(planes, along_x, NN)
    field_x = jnp.zeros((1, atoms), jnp.float32)
    field_y = field_x
    field_z = field_x
    for k in range(freqs):
        wave = wave_ref[0, k : k + 1]
        slope_wave = slope_wave_ref[0, k : k + 1]
        block = probed[k * width_v : (k + 1) * width_v]
        with_slope = block[:, :atoms]
        with_weight = block[:, atoms:]
        field_x += wave * jnp.sum(with_slope * weight_y, 0, keepdims=True)
        field_y += wave * jnp.sum(with_weight * slope_y, 0, keepdims=True)
        field_z += slope_wave * jnp.sum(with_weight * weight_y, 0, keepdims=True)
    out_ref[0, 0:1] = field_x
    out_ref[0, 1:2] = field_y
    out_ref[0, 2:3] = field_z


def z_waves(cell_z, frac_z, freq_z):
    weights, slopes = spline(frac_z)
    turns = 2.0 * math.pi / G
    angle = turns * (cell_z[:, None] * freq_z[None, :, None] % G).astype(jnp.float32)
    cosine, sine = jnp.cos(angle), jnp.sin(angle)
    first = turns * freq_z.astype(jnp.float32)[None, :, None]

    def combined(values):
        values = values[:, :, None]
        even = (
            values[2]
            + (values[1] + values[3]) * jnp.cos(first)
            + (values[0] + values[4]) * jnp.cos(2.0 * first)
        )
        odd = (values[3] - values[1]) * jnp.sin(first) + (values[4] - values[0]) * jnp.sin(
            2.0 * first
        )
        return (cosine + sine) * even + (cosine - sine) * odd

    return combined(weights), combined(slopes)


def padded_length(length):
    return -(-length // 8) * 8


def window_rows(blocks, length):
    width = length + 4
    starts = length * jnp.arange(blocks, dtype=jnp.int32)[:, None]
    spots = jnp.arange(padded_length(width), dtype=jnp.int32)[None]
    points = (starts + spots - 2 + G) % G
    angles = (
        2.0
        * math.pi
        / G
        * (points[:, :, None] * jnp.arange(G, dtype=jnp.int32) % G).astype(jnp.float32)
    )
    return jnp.where((spots < width)[:, :, None], jnp.cos(angles) + jnp.sin(angles), 0.0)


def spread_to_all(values):
    devices = lax.axis_size("slab") * lax.axis_size("space")
    copies = jnp.broadcast_to(values[None], (devices,) + values.shape)
    return lax.all_to_all(copies, ("slab", "space"), split_axis=0, concat_axis=0, tiled=True)


def exchange_sum(fields):
    moved = lax.all_to_all(fields, ("slab", "space"), split_axis=0, concat_axis=0, tiled=True)
    return jnp.sum(moved, 0)


def local(
    dipoles,
    residual,
    cells,
    fraction,
    polarizability,
    tile_order,
    send_tiles,
    tile_lists,
    tile_counts,
):
    atom_order = tile_order[0]
    sending = send_tiles[0]
    neighbour_ids = tile_lists[0]
    counts = tile_counts[0]
    count_tiles = neighbour_ids.shape[0]
    atom_count = atom_order.shape[0]
    send_count = sending.shape[0]
    n_slab = lax.axis_size("slab")
    n_space = lax.axis_size("space")
    extent_x = G // n_slab
    extent_y = G // n_space
    freqs = G // (n_slab * n_space)
    first_freq = (lax.axis_index("slab") * n_space + lax.axis_index("space")) * freqs
    freq_z = first_freq + jnp.arange(freqs, dtype=jnp.int32)
    cell_rows = cells[:, atom_order]
    frac_rows = fraction[:, atom_order]
    alphas = polarizability[atom_order][None]
    target = residual[:, atom_order]
    moments = dipoles[:, atom_order]
    places_all = spread_to_all(jnp.concatenate([cell_rows.astype(jnp.float32), frac_rows], 0))
    cells_all = places_all[:, :3].astype(jnp.int32)
    frac_all = places_all[:, 3:]
    wave_z, slope_wave_z = z_waves(cells_all[:, 2], frac_all[:, 2], freq_z)
    positions = cell_rows.astype(jnp.float32) + frac_rows
    geometry = to_tiles(jnp.concatenate([positions, alphas], 0), count_tiles)
    shift_rows = []
    for step_a in range(3):
        for step_b in range(3):
            if step_a != 1 or step_b != 1:
                shift_rows.append(
                    [float((step_a - 1) * extent_x), float((step_b - 1) * extent_y), 0.0, 0.0]
                )
    shifts = jnp.repeat(jnp.array(shift_rows, jnp.float32), send_count, 0)[:, :, None]
    search = alphas * target
    search_tiles = to_tiles(search, count_tiles)
    first_pool = pool_from(
        tile_rims(jnp.concatenate([geometry, search_tiles], 1)[sending][None, None])
    )
    pool_geometry = jnp.concatenate([geometry, first_pool[:, :4] + shifts], 0)
    coefficients = pair_coefficients(geometry, pool_geometry, neighbour_ids, counts)

    def short_from(values_tiles, received_dipoles):
        pool_dipoles = jnp.concatenate([values_tiles, received_dipoles], 0)
        return from_tiles(
            short_field(geometry, pool_geometry, pool_dipoles, neighbour_ids, coefficients)
        )

    def short_apply(values):
        values_tiles = to_tiles(values, count_tiles)
        return short_from(values_tiles, pool_from(tile_rims(values_tiles[sending][None, None])))

    search = alphas * (target + short_from(search_tiles, first_pool[:, 4:]))
    for sweep_id in range(2):
        search = alphas * (target + short_apply(search))
    search_all = spread_to_all(search)
    window_x = window_rows(n_slab, extent_x).reshape(-1, G)
    window_y = window_rows(n_space, extent_y)
    width_u = padded_length(extent_x + 4)
    width_v = padded_length(extent_y + 4)
    grid_ids = jnp.arange(G, dtype=jnp.int32)
    factor = multiplier(
        grid_ids[None, :, None], grid_ids[None, None, :], freq_z[:, None, None]
    )

    def per_block(rows):
        return pl.BlockSpec((1, rows, atom_count), lambda s, q: (s * n_space + q, 0, 0))

    planes_spec = pl.BlockSpec((freqs, 1, width_u, G), lambda s, q: (0, s, 0, 0))
    cas_spec = pl.BlockSpec((1, width_v, G), lambda s, q: (q, 0, 0))
    along_y = pl.pallas_call(
        spread_kernel,
        grid=(n_slab, n_space),
        in_specs=[
            per_block(3),
            per_block(3),
            per_block(3),
            per_block(freqs),
            per_block(freqs),
            cas_spec,
        ],
        out_specs=planes_spec,
        out_shape=jax.ShapeDtypeStruct((freqs, n_slab, width_u, G), jnp.float32),
        name="spread",
    )(cells_all, frac_all, search_all, wave_z, slope_wave_z, window_y)
    whole = pl.BlockSpec((1, G, G), lambda k: (k, 0, 0))
    planes = pl.BlockSpec((1, n_slab * width_u, G), lambda k: (k, 0, 0))
    back_x, energy = pl.pallas_call(
        scale_kernel,
        grid=(freqs,),
        in_specs=[
            planes,
            pl.BlockSpec(window_x.shape, lambda k: (0, 0)),
            pl.BlockSpec(window_x.shape[::-1], lambda k: (0, 0)),
            whole,
        ],
        out_specs=[planes, pl.BlockSpec((1, 8, G), lambda k: (k, 0, 0))],
        out_shape=[
            jax.ShapeDtypeStruct((freqs, n_slab * width_u, G), jnp.float32),
            jax.ShapeDtypeStruct((freqs, 8, G), jnp.float32),
        ],
        name="scale",
    )(along_y.reshape(freqs, -1, G), window_x, window_x.T, factor)
    direct = search / alphas - short_apply(search) - SELF_FIELD * search
    partial_sums = jnp.stack(
        [jnp.sum(target * search), jnp.sum(search * direct) + jnp.sum(energy[:, 0])]
    )
    totals = jnp.sum(spread_to_all(jnp.broadcast_to(partial_sums[:, None], (2, 128)))[:, :, 0], 0)
    step_size = totals[0] / totals[1]
    fields = pl.pallas_call(
        probe_kernel,
        grid=(n_slab, n_space),
        in_specs=[
            per_block(3),
            per_block(3),
            planes_spec,
            per_block(freqs),
            per_block(freqs),
            cas_spec,
        ],
        out_specs=per_block(3),
        out_shape=jax.ShapeDtypeStruct(cells_all.shape, jnp.float32),
        name="probe",
    )(cells_all, frac_all, back_x.reshape(along_y.shape), wave_z, slope_wave_z, window_y)
    mine = exchange_sum(fields)
    applied = direct + mine

    def restore(values):
        return jnp.zeros_like(values).at[:, atom_order].set(values)

    return (
        restore(moments + step_size * search),
        restore(target - step_size * applied),
        restore(search),
    )


def solution(mesh):
    return jax.shard_map(
        local,
        mesh=mesh,
        in_specs=(
            P(None, ("slab", "space")),
            P(None, ("slab", "space")),
            P(None, ("slab", "space")),
            P(None, ("slab", "space")),
            P(("slab", "space")),
            P(("slab", "space"), None),
            P(("slab", "space"), None),
            P(("slab", "space"), None, None),
            P(("slab", "space"), None),
        ),
        out_specs=(
            P(None, ("slab", "space")),
            P(None, ("slab", "space")),
            P(None, ("slab", "space")),
        ),
        check_vma=False,
    )
```
